8 devices in a mesh: dp: 2 (over z, y), tp: 4 (over x, core).
Axes of the slice: x: 2, y: 2, z: 1, core: 2. Of those that a mesh axis runs over, the one named last changes fastest.
Arguments:
- query: bfloat16 [128, 28, 128], P('dp', 'tp'), parts along dimension 0
- k_cache: bfloat16 [128, 2048, 4, 128], P('dp', None, 'tp'), parts along dimension 0
- v_cache: bfloat16 [128, 2048, 4, 128], P('dp', None, 'tp'), parts along dimension 0
- k_new: bfloat16 [128, 4, 128], P('dp', 'tp'), parts along dimension 0
- v_new: bfloat16 [128, 4, 128], P('dp', 'tp'), parts along dimension 0
- lens: int32 [128], P('dp'), parts along dimension 0
Outputs:
- output 1: bfloat16 [128, 28, 128], P('dp', 'tp'), parts along dimension 0
- output 2: bfloat16 [128, 2048, 4, 128], P('dp', 'tp'), parts along dimension 0
- output 3: bfloat16 [128, 2048, 4, 128], P('dp', 'tp'), parts along dimension 0
There are 2 independent parts. The reference program is written for one: setup_inputs(seed, part) draws one part's arguments, and reference() takes and returns one part's arrays. A program takes and returns all parts, laid end to end along the dimension named above; each array names one.
All inputs are finite; a program needn't handle non-finite values.
Results may differ from the reference program's by a relative error of at most 0.00775914.
Values are sent between devices in bfloat16 or wider.
A program may use at most 1 GiB of HBM per device.

```python
import math
import jax
import jax.numpy as jnp
from jax import lax

BATCH = 64
SEQ_LEN = 2048
Q_HEADS = 28
KV_HEADS = 4
HEAD_DIM = 128


def setup_inputs(seed: int = 0, part: int = 0) -> dict:
    base_key = jax.random.fold_in(jax.random.key(seed), part)
    keys = jax.random.split(base_key, 6)
    group_size = Q_HEADS // KV_HEADS
    spread = math.sqrt(math.log(SEQ_LEN))
    align = 1.4 * math.sqrt(math.log(SEQ_LEN) / HEAD_DIM)
    cache_shape = (BATCH, SEQ_LEN, KV_HEADS, HEAD_DIM)
    k_cache = jax.random.normal(keys[0], cache_shape, jnp.float32)
    v_cache = jax.random.normal(keys[1], cache_shape, jnp.float32)
    k_new = jax.random.normal(keys[2], (BATCH, KV_HEADS, HEAD_DIM), jnp.float32)
    v_new = jax.random.normal(keys[3], (BATCH, KV_HEADS, HEAD_DIM), jnp.float32)
    noise = jax.random.normal(keys[4], (BATCH, KV_HEADS, group_size, HEAD_DIM), jnp.float32)
    mixed = math.sqrt(1.0 - align * align) * noise + align * k_new[:, :, None, :]
    query = (spread * mixed).reshape(BATCH, Q_HEADS, HEAD_DIM)
    len_keys = jax.random.split(keys[5])
    low_len = SEQ_LEN // 8
    lens = jax.random.randint(len_keys[0], (BATCH,), low_len, SEQ_LEN, jnp.int32)
    top_slot = jax.random.randint(len_keys[1], (), 0, BATCH, jnp.int32)
    lens = jnp.where(jnp.arange(BATCH) == top_slot, SEQ_LEN - 1, lens)
    return {"query": query.astype(jnp.bfloat16), "k_cache": k_cache.astype(jnp.bfloat16), "v_cache": v_cache.astype(jnp.bfloat16), "k_new": k_new.astype(jnp.bfloat16), "v_new": v_new.astype(jnp.bfloat16), "lens": lens}


def reference(query, k_cache, v_cache, k_new, v_new, lens):
    positions = jnp.arange(SEQ_LEN, dtype=jnp.int32)
    new_slot = (positions[None, :] == lens[:, None])[:, :, None, None]
    k_upd = jnp.where(new_slot, k_new[:, None], k_cache)
    v_upd = jnp.where(new_slot, v_new[:, None], v_cache)
    group_size = Q_HEADS // KV_HEADS
    inv_sqrt = HEAD_DIM ** -0.5

    def one_head(head_in):
        q_head, k_head, v_head, length = head_in
        scores = jnp.dot(q_head, k_head.T, preferred_element_type=jnp.float32) * inv_sqrt
        scores = jnp.where(positions[None, :] <= length, scores, -1e30)
        probs = jax.nn.softmax(scores, axis=-1)
        return jnp.dot(probs.astype(jnp.bfloat16), v_head, preferred_element_type=jnp.float32)

    q_flat = query.reshape(BATCH * KV_HEADS, group_size, HEAD_DIM)
    k_flat = jnp.swapaxes(k_upd, 1, 2).reshape(BATCH * KV_HEADS, SEQ_LEN, HEAD_DIM)
    v_flat = jnp.swapaxes(v_upd, 1, 2).reshape(BATCH * KV_HEADS, SEQ_LEN, HEAD_DIM)
    len_flat = jnp.repeat(lens, KV_HEADS)
    head_out = lax.map(one_head, (q_flat, k_flat, v_flat, len_flat))
    attn_out = head_out.reshape(BATCH, Q_HEADS, HEAD_DIM).astype(jnp.bfloat16)
    return attn_out, k_upd, v_upd
```

```python
import functools

import jax
import jax.numpy as jnp
from jax import lax
from jax.experimental import pallas as pl
from jax.experimental.pallas import tpu as pltpu
from jax.sharding import PartitionSpec as P


MASK_VALUE = -1e30

CHUNKS = (1, 3, 6, 8, 8, 8, 8, 8, 6, 4, 2, 1, 1)
PEERS = (2, 3, 1)


def prepare_kernel(first, count, seq_part, me_ref, lens_ref, *refs):
    caches, (new_refs), outs = refs[: 2 * count], refs[2 * count : 2 * count + 2], refs[2 * count + 3 : 3 * count + 3]
    new_rows = refs[3 * count + 3 :]
    req = first + pl.program_id(0)
    rows = lax.broadcasted_iota(jnp.int32, caches[0].shape[1:], 0)
    for t in range(2):
        new_rows[t][...] = new_refs[t][...].astype(jnp.float32)
        row = new_rows[t][pl.ds(req, 1), :]
        for i, x in enumerate(PEERS):
            slot = lens_ref[req] - (me_ref[0] ^ x) * seq_part
            piece = caches[t * count + i][0].astype(jnp.float32)
            outs[i][t, 0] = jnp.where(rows == slot, row, piece).astype(jnp.bfloat16)


def prepare(me, lens, k_cache, v_cache, k_new, v_new, token, first, size, seq_part):
    batch, head_dim = k_new.shape
    count = len(PEERS)
    piece = lambda x: pl.BlockSpec((1, seq_part, head_dim), lambda i, me, lens, x=x: (first + i, me[0] ^ x, 0))
    whole = pl.BlockSpec((batch, head_dim), lambda i, me, lens: (0, 0))
    out = pl.BlockSpec((2, 1, seq_part, head_dim), lambda i, me, lens: (0, i, 0, 0))
    return pl.pallas_call(
        functools.partial(prepare_kernel, first, count, seq_part),
        out_shape=[jax.ShapeDtypeStruct((2, size, seq_part, head_dim), jnp.bfloat16)] * count,
        grid_spec=pltpu.PrefetchScalarGridSpec(
            num_scalar_prefetch=2,
            grid=(size,),
            in_specs=[piece(x) for x in PEERS] * 2 + [whole] * 2 + [pl.BlockSpec(memory_space=pl.ANY)],
            out_specs=[out] * count,
            scratch_shapes=[pltpu.VMEM((batch, head_dim), jnp.float32)] * 2,
        ),
        cost_estimate=pl.CostEstimate(flops=10**6 * size, bytes_accessed=12 * size * seq_part * head_dim * 2, transcendentals=0),
    )(me, lens, *[k_cache] * count, *[v_cache] * count, k_new, v_new, token)


def attention_kernel(lens_ref, q_ref, k_ref, v_ref, k_new_ref, v_new_ref, token_ref, out_ref, k_rows, v_rows):
    req = pl.program_id(0)
    k_rows[...] = k_new_ref[...].astype(jnp.float32)
    v_rows[...] = v_new_ref[...].astype(jnp.float32)
    query = q_ref[0]
    scale = query.shape[-1] ** -0.5
    dims = (((1,), (1,)), ((), ()))
    scores = lax.dot_general(query, k_ref[0], dims, preferred_element_type=jnp.float32) * scale
    positions = lax.broadcasted_iota(jnp.int32, scores.shape, 1)
    valid = positions < lens_ref[req]
    scores = jnp.where(valid, scores, MASK_VALUE)
    new_score = jnp.sum(query.astype(jnp.float32) * k_rows[pl.ds(req, 1), :], axis=-1, keepdims=True) * scale
    top = jnp.maximum(jnp.max(scores, axis=-1, keepdims=True), new_score)
    weights = jnp.where(valid, jnp.exp(scores - top), 0.0)
    new_weight = jnp.exp(new_score - top)
    total = jnp.sum(weights, axis=-1, keepdims=True) + new_weight
    probs = (weights / total).astype(jnp.bfloat16)
    new_prob = (new_weight / total).astype(jnp.bfloat16).astype(jnp.float32)
    out = jnp.dot(probs, v_ref[0], preferred_element_type=jnp.float32) + new_prob * v_rows[pl.ds(req, 1), :]
    out_ref[0] = out.astype(jnp.bfloat16)


def attention(lens, query, k_cache, v_cache, k_new, v_new, token):
    batch, seq_len, head_dim = k_cache.shape
    rows = query.shape[1]
    cache = pl.BlockSpec((1, seq_len, head_dim), lambda i, lens: (i, 0, 0))
    heads = pl.BlockSpec((1, rows, head_dim), lambda i, lens: (i, 0, 0))
    whole = pl.BlockSpec((batch, head_dim), lambda i, lens: (0, 0))
    return pl.pallas_call(
        attention_kernel,
        out_shape=jax.ShapeDtypeStruct(query.shape, jnp.bfloat16),
        grid_spec=pltpu.PrefetchScalarGridSpec(
            num_scalar_prefetch=1,
            grid=(batch,),
            in_specs=[heads, cache, cache, whole, whole, pl.BlockSpec(memory_space=pl.ANY)],
            out_specs=heads,
            scratch_shapes=[pltpu.VMEM((batch, head_dim), jnp.float32)] * 2,
        ),
        cost_estimate=pl.CostEstimate(flops=10**8, bytes_accessed=k_cache.size * 4, transcendentals=0),
        name="attention",
    )(lens, query, k_cache, v_cache, k_new, v_new, token)


def interleave_kernel(first, seq_part, n_skip, me_ref, lens_ref, *refs):
    count = len(PEERS)
    owns, pieces, new_refs = refs[:2], refs[2 : 2 + count], refs[2 + count : 4 + count]
    outs, (mixed, *new_rows) = refs[4 + count + n_skip : 6 + count + n_skip], refs[6 + count + n_skip :]
    req = first + pl.program_id(0)
    me = me_ref[0]
    heads = count + 1
    rows = lax.broadcasted_iota(jnp.int32, owns[0].shape[1:], 0)
    slot = lens_ref[req] - me * seq_part
    for t in range(2):
        new_rows[t][...] = new_refs[t][...].astype(jnp.float32)
        row = new_rows[t][pl.ds(req, 1), :]
        mixed[pl.ds(me, seq_part, heads), :] = jnp.where(rows == slot, row, owns[t][0].astype(jnp.float32))
        for i, x in enumerate(PEERS):
            mixed[pl.ds(me ^ x, seq_part, heads), :] = pieces[i][t, 0].astype(jnp.float32)
        outs[t][0] = mixed[...].astype(jnp.bfloat16)


def interleave(me, lens, k_cache, v_cache, pieces, k_new, v_new, bufs, tokens, first, size, seq_part):
    batch, head_dim = k_new.shape
    heads = len(PEERS) + 1
    own = pl.BlockSpec((1, seq_part, head_dim), lambda i, me, lens: (first + i, me[0], 0))
    piece = pl.BlockSpec((2, 1, seq_part, head_dim), lambda i, me, lens: (0, i, 0, 0))
    whole = pl.BlockSpec((batch, head_dim), lambda i, me, lens: (0, 0))
    out = pl.BlockSpec((1, seq_part * heads, head_dim), lambda i, me, lens: (first + i, 0, 0))
    skipped = list(bufs) + list(tokens)
    n_lead = 2 + 2 + len(pieces) + 2
    return pl.pallas_call(
        functools.partial(interleave_kernel, first, seq_part, len(skipped)),
        out_shape=[jax.ShapeDtypeStruct((batch, seq_part * heads, head_dim), jnp.bfloat16)] * 2,
        grid_spec=pltpu.PrefetchScalarGridSpec(
            num_scalar_prefetch=2,
            grid=(size,),
            in_specs=[own] * 2 + [piece] * len(pieces) + [whole] * 2 + [pl.BlockSpec(memory_space=pl.ANY)] * len(skipped),
            out_specs=[out] * 2,
            scratch_shapes=[pltpu.VMEM((seq_part * heads, head_dim), jnp.float32)] + [pltpu.VMEM((batch, head_dim), jnp.float32)] * 2,
        ),
        input_output_aliases={n_lead + i: i for i in range(len(bufs))},
        cost_estimate=pl.CostEstimate(flops=10**6 * size, bytes_accessed=16 * size * seq_part * head_dim * 2, transcendentals=0),
    )(me, lens, k_cache, v_cache, *pieces, k_new, v_new, *skipped)


def solution(mesh):
    n_tp = mesh.shape["tp"]

    def local_step(query, k_cache, v_cache, k_new, v_new, lens):
        batch, seq_len, _, head_dim = k_cache.shape
        seq_part = seq_len // n_tp
        group = query.shape[1]
        me = lax.axis_index("tp").astype(jnp.int32).reshape(1)
        k_cache, v_cache = k_cache.reshape(batch, seq_len, head_dim), v_cache.reshape(batch, seq_len, head_dim)
        k_new, v_new = k_new.reshape(batch, head_dim), v_new.reshape(batch, head_dim)

        token, arrived, first = lens, [], 0
        for size in CHUNKS:
            sends = prepare(me, lens, k_cache, v_cache, k_new, v_new, token, first, size, seq_part)
            pieces = []
            for s, x in zip(sends, PEERS):
                pieces.append(lax.ppermute(s, "tp", [(i, i ^ x) for i in range(n_tp)]))
            arrived.append(pieces)
            token, first = sends[0], first + size

        rows = jnp.pad(query, ((0, 0), (0, 8 - group), (0, 0)))
        attn_out = attention(lens, rows, k_cache, v_cache, k_new, v_new, token)

        bufs, tokens, first = (), (attn_out,), 0
        for size, pieces in zip(CHUNKS, arrived):
            bufs = interleave(me, lens, k_cache, v_cache, pieces, k_new, v_new, bufs, tokens, first, size, seq_part)
            tokens, first = (), first + size
        k_seq, v_seq = (b.reshape(batch, seq_part, n_tp, head_dim) for b in bufs)
        return attn_out[:, :group], k_seq, v_seq

    head_spec = P("dp", "tp")
    entry_spec = P("dp", None, "tp")
    return jax.shard_map(local_step, mesh=mesh, in_specs=(head_spec, entry_spec, entry_spec, head_spec, head_spec, P("dp")), out_specs=(head_spec, P("dp", "tp"), P("dp", "tp")), check_vma=False)
```

```python
import functools

import jax
import jax.numpy as jnp
from jax import lax
from jax.experimental import pallas as pl
from jax.experimental.pallas import tpu as pltpu
from jax.sharding import PartitionSpec as P


FIRST = (63, 1, 1)
CHUNKS = ((0, 4, 4), (4, 36, 4), (40, 20, 4), (60, 2, 2))
LAST = (62, 2, 2)
LAST_SPLIT = (11, 5)
LAST_AFTER = 2
PEERS = (2, 3, 1)
FIRST_PEERS = (PEERS[:1], PEERS[1:])
ROWS = 16
ANY = pl.BlockSpec(memory_space=pl.ANY)


def put_row(ref, index, slot, row):
    @pl.when((slot >= 0) & (slot < ref.shape[-2]))
    def _():
        base = pl.multiple_of((slot // ROWS) * ROWS, ROWS)
        window = (*index, pl.ds(base, ROWS), slice(None))
        old = ref[window].astype(jnp.float32)
        at = lax.broadcasted_iota(jnp.int32, old.shape, 0) == slot - base
        ref[window] = jnp.where(at, row, old).astype(ref.dtype)


def first_kernel(req, size, seq_part, peers, lens_hbm, k_hbm, v_hbm, k_new_hbm, v_new_hbm, *refs):
    outs, (lens, new_rows, sems) = refs[: len(peers)], refs[len(peers) :]
    me = lax.axis_index("tp")
    base = req // ROWS * ROWS
    copies = [pltpu.make_async_copy(lens_hbm, lens, sems.at[0])]
    for t, (cache, new) in enumerate(((k_hbm, k_new_hbm), (v_hbm, v_new_hbm))):
        copies.append(pltpu.make_async_copy(new.at[pl.ds(base, ROWS)], new_rows.at[t], sems.at[1 + t]))
        for i, x in enumerate(peers):
            piece = cache.at[pl.ds(req, size), pl.ds((me ^ x) * seq_part, seq_part)]
            copies.append(pltpu.make_async_copy(piece, outs[i].at[t], sems.at[3 + t * len(peers) + i]))
    for copy in copies:
        copy.start()
    for copy in copies:
        copy.wait()
    for t in range(2):
        for r in range(size):
            row = new_rows[t, pl.ds(req + r - base, 1), :].astype(jnp.float32)
            for i, x in enumerate(peers):
                put_row(outs[i], (t, r), lens[req + r] - (me ^ x) * seq_part, row)


def first_pieces(lens, k_cache, v_cache, k_new, v_new, chunk, peers, make, seq_part):
    first, size, _ = chunk
    head_dim = k_new.shape[-1]
    count = len(peers)
    return pl.pallas_call(
        functools.partial(first_kernel, first, size, seq_part, peers),
        out_shape=[make((2, size, seq_part, head_dim), jnp.bfloat16)] * count,
        in_specs=[ANY] * 5,
        out_specs=[pl.BlockSpec(memory_space=pltpu.VMEM)] * count,
        scratch_shapes=[pltpu.SMEM(lens.shape, jnp.int32), pltpu.VMEM((2, ROWS, head_dim), jnp.bfloat16), pltpu.SemaphoreType.DMA((3 + 2 * count,))],
    )(lens, k_cache, v_cache, k_new, v_new)


def attend_kernel(first, group, seq_part, parts, n_skip, lens_ref, q_ref, k_ref, v_ref, k_new_ref, v_new_ref, *refs):
    (out_ref, *pieces), (k_rows, v_rows) = refs[n_skip:-2], refs[-2:]
    me = lax.axis_index("tp")
    k_rows[...] = k_new_ref[...].astype(jnp.float32)
    v_rows[...] = v_new_ref[...].astype(jnp.float32)
    dims = (((1,), (1,)), ((), ()))
    for r in range(group):
        req = first + pl.program_id(0) * group + r
        length = lens_ref[req]
        for t, (cache, new) in enumerate(((k_ref, k_rows), (v_ref, v_rows))):
            for piece, (x, row0) in zip(pieces, parts):
                if r >= piece.shape[1]:
                    continue
                start = pl.multiple_of((me ^ x) * seq_part + row0, ROWS)
                piece[t, r] = cache[r, pl.ds(start, piece.shape[2]), :]
                put_row(piece, (t, r), length - start, new[pl.ds(req, 1), :])
        query = q_ref[r]
        scale = query.shape[-1] ** -0.5
        scores = lax.dot_general(query, k_ref[r], dims, preferred_element_type=jnp.float32) * scale
        valid = lax.broadcasted_iota(jnp.int32, scores.shape, 1) < length
        scores = jnp.where(valid, scores, -jnp.inf)
        new_score = jnp.sum(query.astype(jnp.float32) * k_rows[pl.ds(req, 1), :], axis=-1, keepdims=True) * scale
        top = jnp.maximum(jnp.max(scores, axis=-1, keepdims=True), new_score)
        weights = jnp.exp(scores - top)
        new_weight = jnp.exp(new_score - top)
        total = jnp.sum(weights, axis=-1, keepdims=True) + new_weight
        probs = (weights / total).astype(jnp.bfloat16)
        new_prob = (new_weight / total).astype(jnp.bfloat16).astype(jnp.float32)
        out = jnp.dot(probs, v_ref[r], preferred_element_type=jnp.float32) + new_prob * v_rows[pl.ds(req, 1), :]
        out_ref[r] = out.astype(jnp.bfloat16)


def attend(lens, query, k_cache, v_cache, k_new, v_new, chunk, ranges, seq_part, n_own=0, buf=(), after=(), sent=0):
    first, size, group = chunk[0] - sent, chunk[1] + sent, chunk[2]
    batch, seq_len, head_dim = k_cache.shape
    rows = query.shape[1]
    parts = [(x, row0, n) for row0, n in ranges for x in PEERS + (0,) * (n_own > 0)]
    at = lambda i, lens: (first // group + i, 0, 0)
    cache = pl.BlockSpec((group, seq_len, head_dim), at)
    heads = pl.BlockSpec((group, rows, head_dim), at)
    whole = pl.BlockSpec((batch, head_dim), lambda i, lens: (0, 0))
    piece = lambda x, n: pl.BlockSpec((2, n_own or group, n, head_dim), lambda i, lens: (0, jnp.maximum(i - sent // group, 0), 0, 0)) if x else pl.BlockSpec(memory_space=pltpu.VMEM)
    shape = lambda x, n: (jax.ShapeDtypeStruct if x else pltpu.VMEM)((2, n_own or size - sent, n, head_dim), jnp.bfloat16)
    return pl.pallas_call(
        functools.partial(attend_kernel, first, group, seq_part, [p[:2] for p in parts], len(buf) + len(after)),
        out_shape=[jax.ShapeDtypeStruct(query.shape, jnp.bfloat16)] + [shape(x, n) for x, _, n in parts],
        grid_spec=pltpu.PrefetchScalarGridSpec(
            num_scalar_prefetch=1,
            grid=(size // group,),
            in_specs=[heads, cache, cache, whole, whole] + [ANY] * (len(buf) + len(after)),
            out_specs=[heads] + [piece(x, n) for x, _, n in parts],
            scratch_shapes=[pltpu.VMEM((batch, head_dim), jnp.float32)] * 2,
        ),
        input_output_aliases={6: 0} if buf else {},
        cost_estimate=pl.CostEstimate(flops=10**6 * size, bytes_accessed=size * seq_len * head_dim * 7, transcendentals=0),
    )(lens, query, k_cache, v_cache, k_new, v_new, *buf, *after)


def interleave_kernel(chunk, n_skip, me_ref, lens_ref, *refs):
    first, _, group = chunk
    count = len(PEERS)
    heads = count + 1
    owns, pieces, new_refs = refs[:2], refs[2 : 2 + count], refs[2 + count : 4 + count]
    outs, (mixed, new_rows) = refs[4 + count + n_skip : 6 + count + n_skip], refs[6 + count + n_skip :]
    me = me_ref[0]
    rows = owns[0].shape[1]

    @pl.loop(0, group)
    def _(r):
        req = first + pl.program_id(0) * group + r
        slot = lens_ref[req] - me * rows
        for t in range(2):
            mixed[pl.ds(me, rows, heads), :] = owns[t][r].astype(jnp.float32)
            for i, x in enumerate(PEERS):
                mixed[pl.ds(me ^ x, rows, heads), :] = pieces[i][t, r].astype(jnp.float32)

            @pl.when((slot >= 0) & (slot < rows))
            def _():
                new_rows[...] = new_refs[t][...].astype(jnp.float32)
                mixed[pl.ds(slot * heads + me, 1), :] = new_rows[pl.ds(req, 1), :]

            outs[t][r] = mixed[...].astype(jnp.bfloat16)


def interleave(me, lens, k_cache, v_cache, pieces, k_new, v_new, bufs, chunk, seq_part):
    first, size, group = chunk
    batch, head_dim = k_new.shape
    heads = len(PEERS) + 1
    own = pl.BlockSpec((group, seq_part, head_dim), lambda i, me, lens: (first // group + i, me[0], 0))
    piece = pl.BlockSpec((2, group, seq_part, head_dim), lambda i, me, lens: (0, i, 0, 0))
    whole = pl.BlockSpec((batch, head_dim), lambda i, me, lens: (0, 0))
    out = pl.BlockSpec((group, seq_part * heads, head_dim), lambda i, me, lens: (first // group + i, 0, 0))
    n_lead = 2 + 2 + len(pieces) + 2
    return pl.pallas_call(
        functools.partial(interleave_kernel, chunk, len(bufs)),
        out_shape=[jax.ShapeDtypeStruct((batch, seq_part * heads, head_dim), jnp.bfloat16)] * 2,
        grid_spec=pltpu.PrefetchScalarGridSpec(
            num_scalar_prefetch=2,
            grid=(size // group,),
            in_specs=[own] * 2 + [piece] * len(pieces) + [whole] * 2 + [ANY] * len(bufs),
            out_specs=[out] * 2,
            scratch_shapes=[pltpu.VMEM((seq_part * heads, head_dim), jnp.float32), pltpu.VMEM((batch, head_dim), jnp.float32)],
        ),
        input_output_aliases={n_lead + i: i for i in range(len(bufs))},
        cost_estimate=pl.CostEstimate(flops=10**6 * size, bytes_accessed=16 * size * seq_part * head_dim * 2, transcendentals=0),
    )(me, lens, k_cache, v_cache, *pieces, k_new, v_new, *bufs)


def last_kernel(req, row0, *refs):
    count = len(PEERS) + 1
    pieces, outs, (mixed, staged, sems) = refs[:count], refs[count + 2 : count + 4], refs[count + 4 :]
    me = lax.axis_index("tp")
    rows = pieces[0].shape[2]
    copies = []
    for t in range(2):
        for piece, x in zip(pieces, PEERS + (0,)):
            mixed[t, pl.ds(me ^ x, rows, count), :] = piece[t, 0].astype(jnp.float32)
        staged[t] = mixed[t].astype(jnp.bfloat16)
        copies.append(pltpu.make_async_copy(staged.at[t], outs[t].at[req, pl.ds(row0 * count, rows * count)], sems.at[t]))
        copies[t].start()
    for copy in copies:
        copy.wait()


def interleave_last(pieces, bufs, row0):
    _, _, rows, head_dim = pieces[0].shape
    count = len(pieces)
    return pl.pallas_call(
        functools.partial(last_kernel, LAST[0], row0),
        out_shape=[jax.ShapeDtypeStruct(b.shape, b.dtype) for b in bufs],
        in_specs=[pl.BlockSpec(memory_space=pltpu.VMEM)] * count + [ANY] * 2,
        out_specs=[ANY] * 2,
        scratch_shapes=[
            pltpu.VMEM((2, rows * count, head_dim), jnp.float32),
            pltpu.VMEM((2, rows * count, head_dim), jnp.bfloat16),
            pltpu.SemaphoreType.DMA((2,)),
        ],
        input_output_aliases={count + i: i for i in range(2)},
        cost_estimate=pl.CostEstimate(flops=10**6, bytes_accessed=16 * rows * head_dim * 2, transcendentals=0),
    )(*(pltpu.with_memory_space_constraint(p, pltpu.VMEM) for p in pieces), *bufs)


def solution(mesh):
    n_tp = mesh.shape["tp"]

    def local_step(query, k_cache, v_cache, k_new, v_new, lens):
        batch, seq_len, _, head_dim = k_cache.shape
        seq_part = seq_len // n_tp
        heads = query.shape[1]
        me = lax.axis_index("tp").astype(jnp.int32).reshape(1)
        k_cache, v_cache = k_cache.reshape(batch, seq_len, head_dim), v_cache.reshape(batch, seq_len, head_dim)
        k_new, v_new = k_new.reshape(batch, head_dim), v_new.reshape(batch, head_dim)
        rows = jnp.pad(query, ((0, 0), (0, 8 - heads), (0, 0)))

        def send(pieces, peers=PEERS):
            moved = []
            for piece, x in zip(pieces, peers):
                moved.append(lax.ppermute(piece, "tp", [(i, i ^ x) for i in range(n_tp)]))
            return moved

        operands = lens, rows, k_cache, v_cache, k_new, v_new
        full = ((0, seq_part),)
        arrived, out = [[]], ()
        for peers in FIRST_PEERS:
            pieces = first_pieces(lens, k_cache, v_cache, k_new, v_new, FIRST, peers, pltpu.VMEM, seq_part)
            arrived[0] += send(pieces, peers)
        for n, chunk in enumerate(CHUNKS, 1):
            if n == 1:
                pieces = first_pieces(lens, k_cache, v_cache, k_new, v_new, chunk, PEERS, jax.ShapeDtypeStruct, seq_part)
            else:
                results = attend(*operands, chunk, full, seq_part, buf=out, sent=CHUNKS[0][1] if n == 2 else 0)
                out, pieces = results[:1], results[1:]
            arrived.append(send(pieces))

        unit = seq_part // sum(LAST_SPLIT)
        ranges = [(sum(LAST_SPLIT[:i]) * unit, share * unit) for i, share in enumerate(LAST_SPLIT)]
        count = len(PEERS) + 1
        out, *pieces = attend(*operands, LAST, ranges, seq_part, 1, out, (arrived[LAST_AFTER][0],))
        last_pieces = []
        for i in range(len(ranges)):
            mine = pieces[i * count : (i + 1) * count]
            last_pieces.append(send(mine[:-1]) + mine[-1:])

        bufs = ()
        for chunk, pieces in zip((FIRST, *CHUNKS), arrived):
            bufs = interleave(me, lens, k_cache, v_cache, pieces, k_new, v_new, bufs, chunk, seq_part)
        for (row0, _), pieces in zip(ranges, last_pieces):
            bufs = interleave_last(pieces, bufs, row0)
        k_seq, v_seq = (b.reshape(batch, seq_part, n_tp, head_dim) for b in bufs)
        return out[:, :heads], k_seq, v_seq

    head_spec = P("dp", "tp")
    entry_spec = P("dp", None, "tp")
    return jax.shard_map(local_step, mesh=mesh, in_specs=(head_spec, entry_spec, entry_spec, head_spec, head_spec, P("dp")), out_specs=(head_spec, P("dp", "tp"), P("dp", "tp")), check_vma=False)
```

```python
import functools

import jax
import jax.numpy as jnp
from jax import lax
from jax.experimental import pallas as pl
from jax.experimental.pallas import tpu as pltpu
from jax.sharding import PartitionSpec as P


FIRST = (63, 1, 1)
CHUNKS = ((0, 4, 4), (4, 36, 4), (40, 20, 4), (60, 2, 2))
LAST = (62, 1, 1)
TAIL = (60, 4, 4)
LAST_SPLIT = (11, 5)
LAST_AFTER = 2
PEERS = (2, 3, 1)
FIRST_PEERS = (PEERS[:1], PEERS[1:])
ROWS = 16
ANY = pl.BlockSpec(memory_space=pl.ANY)


def put_row(ref, index, slot, row):
    @pl.when((slot >= 0) & (slot < ref.shape[-2]))
    def _():
        base = pl.multiple_of((slot // ROWS) * ROWS, ROWS)
        window = (*index, pl.ds(base, ROWS), slice(None))
        old = ref[window].astype(jnp.float32)
        at = lax.broadcasted_iota(jnp.int32, old.shape, 0) == slot - base
        ref[window] = jnp.where(at, row, old).astype(ref.dtype)


def first_kernel(req, size, seq_part, parts, n_skip, lens_hbm, k_hbm, v_hbm, k_new_hbm, v_new_hbm, *refs):
    outs, (lens, new_rows, sems) = refs[n_skip:-3], refs[-3:]
    me = lax.axis_index("tp")
    base = req // ROWS * ROWS
    copies = [pltpu.make_async_copy(lens_hbm, lens, sems.at[0])]
    for t, (cache, new) in enumerate(((k_hbm, k_new_hbm), (v_hbm, v_new_hbm))):
        copies.append(pltpu.make_async_copy(new.at[pl.ds(base, ROWS)], new_rows.at[t], sems.at[1 + t]))
        for i, (x, row0, n) in enumerate(parts):
            piece = cache.at[pl.ds(req, size), pl.ds((me ^ x) * seq_part + row0, n)]
            copies.append(pltpu.make_async_copy(piece, outs[i].at[t], sems.at[3 + t * len(parts) + i]))
    for copy in copies:
        copy.start()
    for copy in copies:
        copy.wait()
    for t in range(2):
        for r in range(size):
            row = new_rows[t, pl.ds(req + r - base, 1), :].astype(jnp.float32)
            for i, (x, row0, _) in enumerate(parts):
                put_row(outs[i], (t, r), lens[req + r] - (me ^ x) * seq_part - row0, row)


def first_pieces(lens, k_cache, v_cache, k_new, v_new, chunk, parts, in_vmem, seq_part, after=()):
    first, size, _ = chunk
    head_dim = k_new.shape[-1]
    count = len(parts)
    return pl.pallas_call(
        functools.partial(first_kernel, first, size, seq_part, parts, len(after)),
        out_shape=[(pltpu.VMEM if in_vmem or not x else jax.ShapeDtypeStruct)((2, size, n, head_dim), jnp.bfloat16) for x, _, n in parts],
        in_specs=[ANY] * (5 + len(after)),
        out_specs=[pl.BlockSpec(memory_space=pltpu.VMEM)] * count,
        scratch_shapes=[pltpu.SMEM(lens.shape, jnp.int32), pltpu.VMEM((2, ROWS, head_dim), jnp.bfloat16), pltpu.SemaphoreType.DMA((3 + 2 * count,))],
    )(lens, k_cache, v_cache, k_new, v_new, *after)


def attend_kernel(first, group, seq_part, parts, n_skip, lens_ref, q_ref, k_ref, v_ref, k_new_ref, v_new_ref, *refs):
    (out_ref, *pieces), (k_rows, v_rows) = refs[n_skip:-2], refs[-2:]
    me = lax.axis_index("tp")
    k_rows[...] = k_new_ref[...].astype(jnp.float32)
    v_rows[...] = v_new_ref[...].astype(jnp.float32)
    dims = (((1,), (1,)), ((), ()))
    for r in range(group):
        req = first + pl.program_id(0) * group + r
        length = lens_ref[req]
        for t, (cache, new) in enumerate(((k_ref, k_rows), (v_ref, v_rows))):
            for piece, (x, row0) in zip(pieces, parts):
                if r >= piece.shape[1]:
                    continue
                start = pl.multiple_of((me ^ x) * seq_part + row0, ROWS)
                piece[t, r] = cache[r, pl.ds(start, piece.shape[2]), :]
                put_row(piece, (t, r), length - start, new[pl.ds(req, 1), :])
        query = q_ref[r]
        scale = query.shape[-1] ** -0.5
        scores = lax.dot_general(query, k_ref[r], dims, preferred_element_type=jnp.float32) * scale
        valid = lax.broadcasted_iota(jnp.int32, scores.shape, 1) < length
        scores = jnp.where(valid, scores, -jnp.inf)
        new_score = jnp.sum(query.astype(jnp.float32) * k_rows[pl.ds(req, 1), :], axis=-1, keepdims=True) * scale
        top = jnp.maximum(jnp.max(scores, axis=-1, keepdims=True), new_score)
        weights = jnp.exp(scores - top)
        new_weight = jnp.exp(new_score - top)
        total = jnp.sum(weights, axis=-1, keepdims=True) + new_weight
        probs = (weights / total).astype(jnp.bfloat16)
        new_prob = (new_weight / total).astype(jnp.bfloat16).astype(jnp.float32)
        out = jnp.dot(probs, v_ref[r], preferred_element_type=jnp.float32) + new_prob * v_rows[pl.ds(req, 1), :]
        out_ref[r] = out.astype(jnp.bfloat16)


def attend(lens, query, k_cache, v_cache, k_new, v_new, chunk, ranges, seq_part, n_sent=0, buf=(), after=(), sent=0):
    first, size, group = chunk[0] - sent, chunk[1] + sent, chunk[2]
    batch, seq_len, head_dim = k_cache.shape
    rows = query.shape[1]
    parts = [(x, row0, n) for row0, n in ranges for x in PEERS]
    at = lambda i, lens: (first // group + i, 0, 0)
    cache = pl.BlockSpec((group, seq_len, head_dim), at)
    heads = pl.BlockSpec((group, rows, head_dim), at)
    whole = pl.BlockSpec((batch, head_dim), lambda i, lens: (0, 0))
    piece = lambda x, n: pl.BlockSpec((2, n_sent or group, n, head_dim), lambda i, lens: (0, jnp.maximum(i - sent // group, 0), 0, 0)) if x else pl.BlockSpec(memory_space=pltpu.VMEM)
    shape = lambda x, n: (jax.ShapeDtypeStruct if x else pltpu.VMEM)((2, n_sent or size - sent, n, head_dim), jnp.bfloat16)
    return pl.pallas_call(
        functools.partial(attend_kernel, first, group, seq_part, [p[:2] for p in parts], len(buf) + len(after)),
        out_shape=[jax.ShapeDtypeStruct(query.shape, jnp.bfloat16)] + [shape(x, n) for x, _, n in parts],
        grid_spec=pltpu.PrefetchScalarGridSpec(
            num_scalar_prefetch=1,
            grid=(size // group,),
            in_specs=[heads, cache, cache, whole, whole] + [ANY] * (len(buf) + len(after)),
            out_specs=[heads] + [piece(x, n) for x, _, n in parts],
            scratch_shapes=[pltpu.VMEM((batch, head_dim), jnp.float32)] * 2,
        ),
        input_output_aliases={6: 0} if buf else {},
        cost_estimate=pl.CostEstimate(flops=10**6 * size, bytes_accessed=size * seq_len * head_dim * 7, transcendentals=0),
    )(lens, query, k_cache, v_cache, k_new, v_new, *buf, *after)


def interleave_kernel(chunk, n_skip, me_ref, lens_ref, *refs):
    first, _, group = chunk
    count = len(PEERS)
    heads = count + 1
    owns, pieces, new_refs = refs[:2], refs[2 : 2 + count], refs[2 + count : 4 + count]
    outs, (mixed, new_rows) = refs[4 + count + n_skip : 6 + count + n_skip], refs[6 + count + n_skip :]
    me = me_ref[0]
    rows = owns[0].shape[1]

    @pl.loop(0, group)
    def _(r):
        req = first + pl.program_id(0) * group + r
        slot = lens_ref[req] - me * rows
        for t in range(2):
            mixed[pl.ds(me, rows, heads), :] = owns[t][r].astype(jnp.float32)
            for i, x in enumerate(PEERS):
                mixed[pl.ds(me ^ x, rows, heads), :] = pieces[i][t, r].astype(jnp.float32)

            @pl.when((slot >= 0) & (slot < rows))
            def _():
                new_rows[...] = new_refs[t][...].astype(jnp.float32)
                mixed[pl.ds(slot * heads + me, 1), :] = new_rows[pl.ds(req, 1), :]

            outs[t][r] = mixed[...].astype(jnp.bfloat16)


def interleave(me, lens, k_cache, v_cache, pieces, k_new, v_new, bufs, chunk, seq_part):
    first, size, group = chunk
    batch, head_dim = k_new.shape
    heads = len(PEERS) + 1
    own = pl.BlockSpec((group, seq_part, head_dim), lambda i, me, lens: (first // group + i, me[0], 0))
    piece = pl.BlockSpec((2, group, seq_part, head_dim), lambda i, me, lens: (0, i, 0, 0))
    whole = pl.BlockSpec((batch, head_dim), lambda i, me, lens: (0, 0))
    out = pl.BlockSpec((group, seq_part * heads, head_dim), lambda i, me, lens: (first // group + i, 0, 0))
    n_lead = 2 + 2 + len(pieces) + 2
    return pl.pallas_call(
        functools.partial(interleave_kernel, chunk, len(bufs)),
        out_shape=[jax.ShapeDtypeStruct((batch, seq_part * heads, head_dim), jnp.bfloat16)] * 2,
        grid_spec=pltpu.PrefetchScalarGridSpec(
            num_scalar_prefetch=2,
            grid=(size // group,),
            in_specs=[own] * 2 + [piece] * len(pieces) + [whole] * 2 + [ANY] * len(bufs),
            out_specs=[out] * 2,
            scratch_shapes=[pltpu.VMEM((seq_part * heads, head_dim), jnp.float32), pltpu.VMEM((batch, head_dim), jnp.float32)],
        ),
        input_output_aliases={n_lead + i: i for i in range(len(bufs))},
        cost_estimate=pl.CostEstimate(flops=10**6 * size, bytes_accessed=16 * size * seq_part * head_dim * 2, transcendentals=0),
    )(me, lens, k_cache, v_cache, *pieces, k_new, v_new, *bufs)


def last_kernel(req, row0, *refs):
    count = len(PEERS) + 1
    pieces, outs, (mixed, staged, sems) = refs[:count], refs[count + 2 : count + 4], refs[count + 4 :]
    me = lax.axis_index("tp")
    rows = pieces[0].shape[2]
    copies = []
    for t in range(2):
        for piece, x in zip(pieces, PEERS + (0,)):
            mixed[t, pl.ds(me ^ x, rows, count), :] = piece[t, 0].astype(jnp.float32)
        staged[t] = mixed[t].astype(jnp.bfloat16)
        copies.append(pltpu.make_async_copy(staged.at[t], outs[t].at[req, pl.ds(row0 * count, rows * count)], sems.at[t]))
        copies[t].start()
    for copy in copies:
        copy.wait()


def interleave_last(pieces, bufs, row0):
    _, _, rows, head_dim = pieces[0].shape
    count = len(pieces)
    return pl.pallas_call(
        functools.partial(last_kernel, LAST[0], row0),
        out_shape=[jax.ShapeDtypeStruct(b.shape, b.dtype) for b in bufs],
        in_specs=[pl.BlockSpec(memory_space=pltpu.VMEM)] * count + [ANY] * 2,
        out_specs=[ANY] * 2,
        scratch_shapes=[
            pltpu.VMEM((2, rows * count, head_dim), jnp.float32),
            pltpu.VMEM((2, rows * count, head_dim), jnp.bfloat16),
            pltpu.SemaphoreType.DMA((2,)),
        ],
        input_output_aliases={count + i: i for i in range(2)},
        cost_estimate=pl.CostEstimate(flops=10**6, bytes_accessed=16 * rows * head_dim * 2, transcendentals=0),
    )(*(pltpu.with_memory_space_constraint(p, pltpu.VMEM) for p in pieces), *bufs)


def solution(mesh):
    n_tp = mesh.shape["tp"]

    def local_step(query, k_cache, v_cache, k_new, v_new, lens):
        batch, seq_len, _, head_dim = k_cache.shape
        seq_part = seq_len // n_tp
        heads = query.shape[1]
        me = lax.axis_index("tp").astype(jnp.int32).reshape(1)
        k_cache, v_cache = k_cache.reshape(batch, seq_len, head_dim), v_cache.reshape(batch, seq_len, head_dim)
        k_new, v_new = k_new.reshape(batch, head_dim), v_new.reshape(batch, head_dim)
        rows = jnp.pad(query, ((0, 0), (0, 8 - heads), (0, 0)))

        def send(pieces, peers=PEERS):
            moved = []
            for piece, x in zip(pieces, peers):
                moved.append(lax.ppermute(piece, "tp", [(i, i ^ x) for i in range(n_tp)]))
            return moved

        operands = lens, rows, k_cache, v_cache, k_new, v_new
        full = ((0, seq_part),)
        arrived, out = [[]], ()
        for peers in FIRST_PEERS:
            pieces = first_pieces(lens, k_cache, v_cache, k_new, v_new, FIRST, [(x, 0, seq_part) for x in peers], True, seq_part)
            arrived[0] += send(pieces, peers)
        for n, chunk in enumerate(CHUNKS, 1):
            if n == 1:
                pieces = first_pieces(lens, k_cache, v_cache, k_new, v_new, chunk, [(x, 0, seq_part) for x in PEERS], False, seq_part)
            else:
                results = attend(*operands, TAIL if n == len(CHUNKS) else chunk, full, seq_part, chunk[1] if n == len(CHUNKS) else 0, out, (), CHUNKS[0][1] if n == 2 else 0)
                out, pieces = results[:1], results[1:]
            arrived.append(send(pieces))

        unit = seq_part // sum(LAST_SPLIT)
        ranges = [(sum(LAST_SPLIT[:i]) * unit, share * unit) for i, share in enumerate(LAST_SPLIT)]
        count = len(PEERS) + 1
        parts = [(x, row0, share) for row0, share in ranges for x in PEERS + (0,)]
        pieces = list(first_pieces(lens, k_cache, v_cache, k_new, v_new, LAST, parts, False, seq_part, (arrived[LAST_AFTER][0],)))
        last_pieces = []
        for i in range(len(ranges)):
            mine = pieces[i * count : (i + 1) * count]
            last_pieces.append(send(mine[:-1]) + mine[-1:])

        bufs = ()
        for chunk, pieces in zip((FIRST, *CHUNKS), arrived):
            bufs = interleave(me, lens, k_cache, v_cache, pieces, k_new, v_new, bufs, chunk, seq_part)
        for (row0, _), pieces in zip(ranges, last_pieces):
            bufs = interleave_last(pieces, bufs, row0)
        k_seq, v_seq = (b.reshape(batch, seq_part, n_tp, head_dim) for b in bufs)
        return out[0][:, :heads], k_seq, v_seq

    head_spec = P("dp", "tp")
    entry_spec = P("dp", None, "tp")
    return jax.shard_map(local_step, mesh=mesh, in_specs=(head_spec, entry_spec, entry_spec, head_spec, head_spec, P("dp")), out_specs=(head_spec, P("dp", "tp"), P("dp", "tp")), check_vma=False)
```
